32 devices in a mesh: row: 4 (over z), col: 4 (over x, core), mp: 2 (over y).
Axes of the slice: x: 2, y: 2, z: 4, core: 2. Of those that a mesh axis runs over, the one named last changes fastest.
Arguments:
- weights: bfloat16 [4, 4, 5, 2304, 1024], P('row', 'col', None, None, 'mp'), may hold values from -6 to 6
- warm_down: bfloat16 [4, 4, 5, 4, 1024], P('row', 'col', None, None, 'mp'), may hold values from -6 to 6
- warm_right: bfloat16 [4, 4, 5, 4, 1024], P('row', 'col', None, None, 'mp'), may hold values from -6 to 6
Outputs:
- new_weights: bfloat16 [4, 4, 5, 2304, 1024], P('row', 'col', None, None, 'mp')
- next_down: float32 [4, 4, 5, 4, 1024], P('row', 'col', None, None, 'mp')
- next_right: float32 [4, 4, 5, 4, 1024], P('row', 'col', None, None, 'mp')
The draws below stay inside these ranges and needn't reach their ends.
All inputs are finite; a program needn't handle non-finite values.
Results may differ from the reference program's by a relative error of at most 0.0085.
Values may be sent and summed in bfloat16 or wider, within the bound.
A program may use at most 128 MiB of HBM per device.

```python
import jax
import jax.numpy as jnp
from jax import lax

D = 2304
KVW = 1024
RANK = 4
LAYERS = 5
ROUNDS = 2
GRID_ROWS = 4
GRID_COLS = 4


def block_levels(key, dims, shards, smallest, high):
    factor_of, own = 1.0, jax.random.fold_in(key, 6)
    for dim, shards_of in shards:
        heights = jnp.exp(jax.random.uniform(jax.random.fold_in(own, dim), (shards_of,), jnp.float32, smallest / len(shards), high / len(shards)))
        factor_of = factor_of * jnp.repeat(heights, dims[dim] // shards_of).reshape([-1 if axis == dim else 1 for axis in range(len(dims))])
    return factor_of


def scatter_about(key, extent, width, bound, split=(), held_as=jnp.bfloat16):
    level = block_levels(key, extent, split, -0.22, 0.18) if split else 1.0
    array = jax.random.normal(key, extent, jnp.float32) * width * level
    return jnp.minimum(jnp.maximum(array, -bound), bound).astype(held_as)


def setup_inputs(seed: int = 0) -> dict:
    arg_keys = jax.random.split(jax.random.key(seed), 4)
    weights = scatter_about(arg_keys[0], (GRID_ROWS, GRID_COLS, LAYERS, D, KVW), 1.0, 6.0, ((0, 4), (1, 4), (4, 2)))
    warm_down = scatter_about(arg_keys[1], (GRID_ROWS, GRID_COLS, LAYERS, RANK, KVW), 1.0, 6.0, ((0, 4), (1, 4), (4, 2)))
    warm_right = scatter_about(arg_keys[2], (GRID_ROWS, GRID_COLS, LAYERS, RANK, KVW), 1.0, 6.0, ((0, 4), (1, 4), (4, 2)))
    return {"weights": weights, "warm_down": warm_down, "warm_right": warm_right}


step_size = 0.2
epsilon = 1e-06

def orthonormal(vectors):
    basis = []
    for column in range(vectors.shape[-2]):
        source = vectors[..., column, :]
        update = source
        for earlier in basis:
            update = update - lax.optimization_barrier(jnp.sum(source * earlier, axis=-1, keepdims=True)) * earlier
        basis.append(update / jnp.sqrt(lax.optimization_barrier(jnp.sum(update * update, axis=-1, keepdims=True)) + epsilon))
    return jnp.stack(basis, axis=-2)

def forward_products(layer_x, factors):

    def single(operands):
        return jnp.dot(operands[1], operands[0].T, preferred_element_type=jnp.float32)
    return lax.map(single, (layer_x, factors))

def backward_products(layer_x, basis):

    def single(operands):
        return jnp.dot(operands[1], operands[0], preferred_element_type=jnp.float32)
    return lax.map(single, (layer_x, basis))

def apply_update(layer_x, basis, factors):

    def single(triple):
        correction = jnp.dot(triple[1].T, triple[2], preferred_element_type=jnp.float32)
        return (triple[0].astype(jnp.float32) - step_size * correction).astype(jnp.bfloat16)
    return lax.map(single, (layer_x, basis, factors))

def one_round(layer_x, down_q, right_q):
    node_count = GRID_ROWS * GRID_COLS
    flat_x = layer_x.reshape(node_count, D, KVW)

    def to_grid(values):
        return values.reshape(GRID_ROWS, GRID_COLS, values.shape[1], values.shape[2])

    def to_flat(values):
        return values.reshape(node_count, values.shape[2], values.shape[3])
    stacked = jnp.concatenate([down_q, right_q, jnp.roll(down_q, 1, 0), jnp.roll(right_q, 1, 1)], axis=2)
    forward = to_grid(forward_products(flat_x, to_flat(stacked)))
    down_diff = forward[:, :, :RANK] - jnp.roll(forward[:, :, 2 * RANK:3 * RANK], -1, 0)
    right_diff = forward[:, :, RANK:2 * RANK] - jnp.roll(forward[:, :, 3 * RANK:], -1, 1)
    down_p = orthonormal(down_diff).astype(jnp.bfloat16)
    right_p = orthonormal(right_diff).astype(jnp.bfloat16)
    basis = jnp.concatenate([down_p, right_p, jnp.roll(down_p, 1, 0), jnp.roll(right_p, 1, 1)], axis=2)
    backward = to_grid(backward_products(flat_x, to_flat(basis)))
    down_c = backward[:, :, :RANK] - jnp.roll(backward[:, :, 2 * RANK:3 * RANK], -1, 0)
    right_c = backward[:, :, RANK:2 * RANK] - jnp.roll(backward[:, :, 3 * RANK:], -1, 1)
    down_next = down_c.astype(jnp.bfloat16)
    right_next = right_c.astype(jnp.bfloat16)
    own_basis = jnp.concatenate([down_p, right_p, -jnp.roll(down_p, 1, 0), -jnp.roll(right_p, 1, 1)], axis=2)
    own_factors = jnp.concatenate([down_next, right_next, jnp.roll(down_next, 1, 0), jnp.roll(right_next, 1, 1)], axis=2)
    new_x = apply_update(flat_x, to_flat(own_basis), to_flat(own_factors)).reshape(layer_x.shape)
    return (new_x, down_next, right_next, down_c, right_c)

def reference(weights, warm_down, warm_right):
    new_layers = []
    downs = []
    rights = []
    for level_index in range(LAYERS):
        layer_x = weights[:, :, level_index]
        down_q = warm_down[:, :, level_index]
        right_q = warm_right[:, :, level_index]
        down_c = jnp.zeros(down_q.shape, jnp.float32)
        right_c = jnp.zeros(right_q.shape, jnp.float32)
        for repeat in range(ROUNDS):
            layer_x, down_q, right_q, down_c, right_c = one_round(layer_x, down_q, right_q)
        new_layers.append(layer_x)
        downs.append(down_c)
        rights.append(right_c)
    return (jnp.stack(new_layers, 2), jnp.stack(downs, 2), jnp.stack(rights, 2))
```

```python
import functools

import jax
import jax.numpy as jnp
from jax import lax
from jax.experimental import pallas as pl
from jax.experimental.pallas import tpu as pltpu
from jax.sharding import PartitionSpec as P

ROUNDS = 2

step_size = 0.2
epsilon = 1e-06

MESH = pl.DeviceIdType.MESH
F32 = jnp.float32
BF16 = jnp.bfloat16
EDGES = 4


def piece(total, want):
    size = min(total, want)
    while total % size:
        size -= 128
    return size


def orthonormal_pairs(v, rank):
    row = lax.broadcasted_iota(jnp.int32, (v.shape[0], 1), 0)
    first = row < rank
    within = jnp.where(first, row, row - rank)
    u = v
    scale = jnp.zeros(row.shape, F32)
    for j in range(rank):
        source = jnp.where(first, u[j : j + 1], u[rank + j : rank + j + 1])
        norm = jnp.sum(source * source, axis=-1, keepdims=True)
        inverse = 1.0 / jnp.sqrt(norm + epsilon)
        scale = jnp.where(within == j, inverse, scale)
        if j + 1 < rank:
            dots = jnp.sum(v * source, axis=-1, keepdims=True)
            u = u - jnp.where(within > j, dots * inverse * inverse, 0.0) * source
    return u * scale


COST = {"own": 0.65, "far": 0.65, "forward": 0.8, "mid": 0.07, "basis": 0.9, "combine": 0.1}
ROW, COL, PART, WIRE = 3.8, 2.9, 2.6, 0.33
ENDS = {0: 0, 1: 2}


def plan(layers):
    def order(r, l):
        return "ends" if l >= layers - ENDS[r] else "sum"

    wire, now, done = 0.0, 0.0, []
    ready = {("own", 0, l, 0): 2.2 + 0.4 * l for l in range(layers)}
    ready.update({("far", 0, l, 0): 6.1 for l in range(layers)})
    arrived = {}
    rank_of = {"mid": 0, "combine": 1, "basis": 2, "forward": 3, "far": 4, "own": 5}

    def hop(e):
        return ROW if e % 2 == 0 else COL

    def across(t):
        nonlocal wire
        wire = max(wire, t) + WIRE
        return wire + PART

    def sent(r, l, e, t):
        first = across(t) if order(r, l) == "sum" else t + hop(e)
        ready["mid", r, l, e] = first

    while ready:
        soon = [k for k, t in ready.items() if t <= now]
        if soon:
            key = min(soon, key=lambda k: (rank_of[k[0]], ready[k], k))
        else:
            key = min(ready, key=lambda k: (ready[k], k))
        name, r, l, e = key
        now = max(now, ready.pop(key)) + COST[name]
        done.append(key)
        if name == "own":
            for i in (0, 1):
                sent(r, l, i, now)
        elif name == "far":
            for i in (2, 3):
                sent(r, l, i, now)
        elif name == "forward":
            for i in (0, 2, 1, 3):
                sent(r, l, i, now)
        elif name == "mid":
            last = now + hop(e) if order(r, l) == "sum" else across(now)
            got = arrived.setdefault((r, l), [])
            got.append(last)
            if len(got) == EDGES:
                ready["basis", r, l, 0] = max(got)
        elif name == "basis":
            ready["combine", r, l, 0] = now + ROW
        elif r + 1 < ROUNDS:
            ready["forward", r + 1, l, 0] = now
    return [(name, r, l, e, order(r, l)) for name, r, l, e in done]


def gossip_kernel(
    sizes, w_hbm, down_hbm, right_hbm, w, p_out, s_out, c_out,
    warm, warm_in, q, kept, vs, vr, ms, mr, cs, cr,
    load_sem, warm_load, warm_send, warm_recv, v_send, v_recv,
    m_send, m_recv, c_send, c_recv,
):
    rows, cols, parts = sizes
    layers, d, k = w_hbm.shape
    rank = down_hbm.shape[1]
    half = 2 * rank
    full = EDGES * rank
    row, col, part = (lax.axis_index(a) for a in ("row", "col", "mp"))
    below = {"row": lax.rem(row + 1, rows)}
    above = {"row": lax.rem(row + rows - 1, rows)}
    right = {"col": lax.rem(col + 1, cols)}
    left = {"col": lax.rem(col + cols - 1, cols)}
    peers = [{"mp": lax.rem(part + i, parts)} for i in range(1, parts)]
    sides = (below, right, above, left)

    def load(l):
        return pltpu.make_async_copy(w_hbm.at[l], w.at[l], load_sem.at[l])

    def warm_loads():
        return [
            pltpu.make_async_copy(src, warm.at[i], warm_load.at[i])
            for i, src in enumerate((down_hbm, right_hbm))
        ]

    def remote(src, dst, send, recv, target):
        return pltpu.make_async_remote_copy(
            src_ref=src, dst_ref=dst, send_sem=send, recv_sem=recv,
            device_id=target, device_id_type=MESH,
        )

    def warm_copies():
        return [
            remote(warm.at[0], warm_in.at[0], warm_send.at[0], warm_recv.at[0], below),
            remote(warm.at[1], warm_in.at[1], warm_send.at[1], warm_recv.at[1], right),
        ]

    def m_copies(r, l, e):
        return [
            remote(
                ms.at[r, l, e], mr.at[r, l, i, e],
                m_send.at[r, l, i, e], m_recv.at[r, l, i, e], t,
            )
            for i, t in enumerate(peers)
        ]

    def edge_copy(src, dst, send, recv, r, l, e):
        o = (e + 2) % EDGES
        return remote(src.at[r, l, e], dst.at[r, l, o], send.at[r, l, e], recv.at[r, l, o], sides[e])

    def edge_wait(src, dst, send, recv, r, l, e):
        remote(
            src.at[r, l, e], dst.at[r, l, e], send.at[r, l, e], recv.at[r, l, e], sides[e]
        ).wait_recv()

    v_refs = (vs, vr, v_send, v_recv)
    c_refs = (cs, cr, c_send, c_recv)

    def each_layer(stage):
        def step(l, carry):
            stage(l)
            return carry
        lax.fori_loop(0, layers, step, 0)

    for copy in warm_loads():
        copy.start()
    each_layer(lambda l: load(l).start())
    barrier = pltpu.get_barrier_semaphore()
    partners = list(sides) + peers
    for t in partners:
        pl.semaphore_signal(barrier, inc=1, device_id=t, device_id_type=MESH)
    pl.semaphore_wait(barrier, len(partners))
    for copy in warm_loads():
        copy.wait()
    for copy in warm_copies():
        copy.start()

    width = piece(d, 768)

    def rows_of(e):
        return slice(e * rank, (e + 1) * rank)

    def launch(r, l, order, edges):
        for e in edges:
            if order == "sum":
                for copy in m_copies(r, l, e):
                    copy.start()
            else:
                edge_copy(*v_refs, r, l, e).start()

    def products(r, l, order, factors, edges, extra=None):
        out = ms if order == "sum" else vs
        for at in range(0, d, width):
            cut = slice(at, at + width)
            f = lax.dot_general(
                factors, w[l, cut, :], (((1,), (1,)), ((), ())), preferred_element_type=F32
            )
            if extra is not None:
                f = f + jnp.dot(extra, p_out[l, 0:full, cut], preferred_element_type=F32)
            first = edges[0] * rank
            kept[l, first : first + len(edges) * rank, cut] = f
            for i, e in enumerate(edges):
                out[r, l, e, :, cut] = f[rows_of(i)].astype(BF16)

    def own(r, l, e, order):
        load(l).wait()
        products(r, l, order, jnp.concatenate([warm[0, l], warm[1, l]], axis=0), (0, 1))
        launch(r, l, order, (0, 1))

    def far(r, l, e, order):
        if waiting:
            for copy in warm_copies():
                copy.wait_recv()
            waiting.clear()
        products(r, l, order, jnp.concatenate([warm_in[0, l], warm_in[1, l]], axis=0), (2, 3))
        launch(r, l, order, (2, 3))

    def forward(r, l, e, order):
        g = lax.dot_general(
            q[l], s_out[l, 0:full], (((1,), (1,)), ((), ())), preferred_element_type=F32
        )
        products(r, l, order, q[l], (0, 1, 2, 3), g.astype(BF16))
        launch(r, l, order, (0, 2, 1, 3))

    def mid(r, l, e, order):
        here = rows_of(e)
        if order == "sum":
            for copy in m_copies(r, l, e):
                copy.wait_recv()
            v = kept[l, here]
            for i in range(len(peers)):
                v = v + mr[r, l, i, e].astype(F32)
            kept[l, here] = v
            vs[r, l, e] = v.astype(BF16)
            edge_copy(*v_refs, r, l, e).start()
        else:
            edge_wait(*v_refs, r, l, e)
            other = vr[r, l, e].astype(F32)
            v = kept[l, here] - other if e < 2 else other - kept[l, here]
            kept[l, here] = v
            ms[r, l, e] = v.astype(BF16)
            for copy in m_copies(r, l, e):
                copy.start()

    def basis(r, l, e, order):
        for i in range(EDGES):
            if order == "sum":
                edge_wait(*v_refs, r, l, i)
            else:
                for copy in m_copies(r, l, i):
                    copy.wait_recv()
        for h in range(2):
            pair = (2 * h, 2 * h + 1)
            v = kept[l, half * h : half * (h + 1)]
            if order == "sum":
                other = jnp.concatenate([vr[r, l, i].astype(F32) for i in pair], axis=0)
                v = v - other if h == 0 else other - v
            else:
                for j in range(len(peers)):
                    v = v + jnp.concatenate([mr[r, l, j, i].astype(F32) for i in pair], axis=0)
            at = r * full + half * h
            p_out[l, at : at + half] = orthonormal_pairs(v, rank).astype(BF16)
        p = p_out[l, r * full : (r + 1) * full]
        b = jnp.dot(p, w[l], preferred_element_type=F32)
        for o in range(r):
            before = slice(o * full, (o + 1) * full)
            g = lax.dot_general(
                p, p_out[l, before], (((1,), (1,)), ((), ())), preferred_element_type=F32
            )
            b = b + jnp.dot(g.astype(BF16), s_out[l, before], preferred_element_type=F32)
        for i in range(EDGES):
            cs[r, l, i] = b[rows_of(i)]
        for i in (0, 2, 1, 3):
            edge_copy(*c_refs, r, l, i).start()

    def combine(r, l, e, order):
        for i in range(EDGES):
            edge_wait(*c_refs, r, l, i)
        mine = [cs[r, l, i] - cr[r, l, i] for i in range(2)]
        theirs = [cr[r, l, i] - cs[r, l, i] for i in range(2, EDGES)]
        if r == ROUNDS - 1:
            for i in range(2):
                c_out[i, l] = mine[i]
        else:
            q[l] = jnp.concatenate(mine + theirs, axis=0).astype(BF16)
        signed = jnp.concatenate([-x for x in mine] + theirs, axis=0)
        s_out[l, r * full : (r + 1) * full] = (step_size * signed).astype(BF16)

    waiting = [True]
    stages = dict(own=own, far=far, forward=forward, mid=mid, basis=basis, combine=combine)
    for name, r, l, e, order in plan(layers):
        stages[name](r, l, e, order)

    for copy in warm_copies():
        copy.wait_send()

    def finish(l):
        for r in range(ROUNDS):
            for e in range(EDGES):
                for copy in m_copies(r, l, e):
                    copy.wait_send()
                edge_copy(*v_refs, r, l, e).wait_send()
                edge_copy(*c_refs, r, l, e).wait_send()

    each_layer(finish)


def gossip(sizes, layers, warm_down, warm_right):
    count, d, k = layers.shape
    rank = warm_down.shape[1]
    others = sizes[2] - 1
    full = EDGES * rank
    vmem = pl.BlockSpec(memory_space=pltpu.VMEM)
    hbm = pl.BlockSpec(memory_space=pltpu.HBM)
    dma = pltpu.SemaphoreType.DMA
    lead = (ROUNDS, count)
    return pl.pallas_call(
        functools.partial(gossip_kernel, sizes),
        out_shape=(
            jax.ShapeDtypeStruct((count, d, k), BF16),
            jax.ShapeDtypeStruct((count, ROUNDS * full, d), BF16),
            jax.ShapeDtypeStruct((count, ROUNDS * full, k), BF16),
            jax.ShapeDtypeStruct((2, count, rank, k), F32),
        ),
        in_specs=[hbm, hbm, hbm],
        out_specs=(vmem, vmem, vmem, vmem),
        scratch_shapes=[
            pltpu.VMEM((2, count, rank, k), BF16),
            pltpu.VMEM((2, count, rank, k), BF16),
            pltpu.VMEM((count, full, k), BF16),
            pltpu.VMEM((count, full, d), F32),
            pltpu.VMEM(lead + (EDGES, rank, d), BF16),
            pltpu.VMEM(lead + (EDGES, rank, d), BF16),
            pltpu.VMEM(lead + (EDGES, rank, d), BF16),
            pltpu.VMEM(lead + (others, EDGES, rank, d), BF16),
            pltpu.VMEM(lead + (EDGES, rank, k), F32),
            pltpu.VMEM(lead + (EDGES, rank, k), F32),
            dma((count,)),
            dma((2,)),
            dma((2,)),
            dma((2,)),
            dma(lead + (EDGES,)),
            dma(lead + (EDGES,)),
            dma(lead + (others, EDGES)),
            dma(lead + (others, EDGES)),
            dma(lead + (EDGES,)),
            dma(lead + (EDGES,)),
        ],
        compiler_params=pltpu.CompilerParams(
            collective_id=0, has_side_effects=True, vmem_limit_bytes=40 * 2**20
        ),
    )(layers, warm_down, warm_right)


def finish_kernel(w, p, s, c, out, down, right, held, out_sem, c_sem):
    layers, d, k = w.shape
    height = piece(d, 256)
    block = piece(d, 768)
    small = [
        pltpu.make_async_copy(c.at[i], dst, c_sem.at[i]) for i, dst in enumerate((down, right))
    ]
    for copy in small:
        copy.start()

    def store(l, b):
        span = pl.ds(b * block, block)
        return pltpu.make_async_copy(held.at[l, span], out.at[l, span], out_sem.at[l, b])

    for l in range(layers):
        for b in range(d // block):
            for at in range(b * block, (b + 1) * block, height):
                cut = slice(at, at + height)
                change = lax.dot_general(
                    p[l, :, cut], s[l], (((0,), (0,)), ((), ())), preferred_element_type=F32
                )
                held[l, cut, :] = (w[l, cut, :].astype(F32) + change).astype(BF16)
            store(l, b).start()
    for copy in small:
        copy.wait()
    for l in range(layers):
        for b in range(d // block):
            store(l, b).wait()


def last_update(w0, basis, factors, combined):
    count, d, k = w0.shape
    rank = combined.shape[2]
    vmem = pl.BlockSpec(memory_space=pltpu.VMEM)
    hbm = pl.BlockSpec(memory_space=pltpu.HBM)
    dma = pltpu.SemaphoreType.DMA
    return pl.pallas_call(
        finish_kernel,
        out_shape=(
            jax.ShapeDtypeStruct((count, d, k), BF16),
            jax.ShapeDtypeStruct((count, rank, k), F32),
            jax.ShapeDtypeStruct((count, rank, k), F32),
        ),
        in_specs=[vmem, vmem, vmem, vmem],
        out_specs=(hbm, hbm, hbm),
        scratch_shapes=[
            pltpu.VMEM((count, d, k), BF16),
            dma((count, d // piece(d, 768))),
            dma((2,)),
        ],
        compiler_params=pltpu.CompilerParams(vmem_limit_bytes=24 * 2**20),
    )(w0, basis, factors, combined)


def solution(mesh):
    sizes = tuple(mesh.shape[a] for a in ("row", "col", "mp"))

    def body(weights, warm_down, warm_right):
        parts = gossip(sizes, weights[0, 0], warm_down[0, 0], warm_right[0, 0])
        new, down, right = last_update(*parts)
        return new[None, None], down[None, None], right[None, None]

    spec = P("row", "col", None, None, "mp")
    return jax.shard_map(
        body, mesh=mesh, in_specs=(spec,) * 3, out_specs=(spec,) * 3, check_vma=False
    )
```

```python
import functools

import jax
import jax.numpy as jnp
from jax import lax
from jax.experimental import pallas as pl
from jax.experimental.pallas import tpu as pltpu
from jax.sharding import PartitionSpec as P

ROUNDS = 2

step_size = 0.2
epsilon = 1e-06

MESH = pl.DeviceIdType.MESH
F32 = jnp.float32
BF16 = jnp.bfloat16
EDGES = 4


def piece(total, want):
    size = min(total, want)
    while total % size:
        size -= 128
    return size


def total(values):
    return functools.reduce(lambda a, b: a + b, values)


def orthonormal_pairs(v, rank):
    row = lax.broadcasted_iota(jnp.int32, (v.shape[0], 1), 0)
    first = row < rank
    within = jnp.where(first, row, row - rank)
    turned = [v] + [pltpu.roll(v, s, 0) for s in range(1, rank)]
    inner = [jnp.sum(v * t, axis=-1, keepdims=True) for t in turned]

    def pick(k, j):
        k, j = max(k, j), min(k, j)
        dots = inner[k - j]
        return jnp.where(first, dots[k : k + 1], dots[rank + k : rank + k + 1])

    gram = [[pick(k, j) for j in range(rank)] for k in range(rank)]
    mix, inverse = [], []
    for k in range(rank):
        ahead = [
            total([mix[j][i] * gram[k][i] for i in range(j)] + [gram[k][j]])
            * (inverse[j] * inverse[j])
            for j in range(k)
        ]
        mix.append([
            -total([ahead[j] * mix[j][i] for j in range(i + 1, k)] + [ahead[i]])
            for i in range(k)
        ])
        along = [
            total([mix[k][i] * gram[i][j] for i in range(k)] + [gram[k][j]])
            for j in range(k + 1)
        ]
        norm = total([mix[k][j] * along[j] for j in range(k)] + [along[k]])
        inverse.append(lax.rsqrt(jnp.maximum(norm, 0.0) + epsilon))
    out = None
    for s in range(rank):
        weight = jnp.zeros(row.shape, F32)
        for k in range(s, rank):
            entry = inverse[k] if s == 0 else inverse[k] * mix[k][k - s]
            weight = jnp.where(within == k, entry, weight)
        out = weight * turned[s] if s == 0 else out + weight * turned[s]
    return out


COST = {
    "own": 0.79, "far": 0.78, "forward": 0.95, "mid": 0.05, "basis": 0.7, "combine": 0.05,
    "update": 0.85,
}
ROW, COL, PART, ACROSS, ALONG = 3.2, 2.4, 2.4, 0.4, 0.4
ENDS = {0: 0, 1: 2}
RANKED = ("mid", "combine", "basis", "forward", "far", "own", "update")


def plan(layers):
    def order(r, l):
        return "ends" if l >= layers - ENDS[r] else "sum"

    wires = {}
    now, done = 0.0, []
    ready = {("own", 0, l, 0): 2.2 + 0.4 * l for l in range(layers)}
    ready.update({("far", 0, l, 0): 6.0 for l in range(layers)})
    arrived = {}

    def over(wire, t, size, latency):
        wires[wire] = max(wires.get(wire, 0.0), t) + size
        return wires[wire] + latency

    def hop(e, t):
        return over(("row", e), t, ALONG, ROW) if e % 2 == 0 else t + COL

    def across(t):
        return over("mp", t, ACROSS, PART)

    def sent(r, l, edges, t):
        for e in edges:
            ready["mid", r, l, e] = across(t) if order(r, l) == "sum" else hop(e, t)

    while ready:
        soon = [k for k, t in ready.items() if t <= now]
        if soon:
            key = min(soon, key=lambda k: (RANKED.index(k[0]), ready[k], k))
        else:
            key = min(ready, key=lambda k: (ready[k], k))
        name, r, l, e = key
        now = max(now, ready.pop(key)) + COST[name]
        done.append(key)
        if name == "own":
            sent(r, l, (0, 1), now)
        elif name == "far":
            sent(r, l, (2, 3), now)
        elif name == "forward":
            sent(r, l, (0, 2, 1, 3), now)
            ready["update", r, l, 0] = now
        elif name == "mid":
            got = arrived.setdefault((r, l), [])
            got.append(hop(e, now) if order(r, l) == "sum" else across(now))
        elif name == "basis":
            ready["combine", r, l, 0] = now + ROW + 0.4
        elif name == "combine" and r + 1 < ROUNDS:
            ready["forward", r + 1, l, 0] = now
        if len(arrived.get((r, l), ())) == EDGES and (r == 0 or ("update", r, l, 0) in done):
            if ("basis", r, l, 0) not in done:
                ready["basis", r, l, 0] = max(arrived[r, l])
    return [(name, r, l, e, order(r, l)) for name, r, l, e in done]


def gossip_kernel(
    sizes, w_hbm, down_hbm, right_hbm, w, p_out, s_out, c_out,
    warm, warm_in, q, kept, held, vs, vr, ms, mr, cs, cr,
    load_sem, warm_load, warm_send, warm_recv, v_send, v_recv,
    m_send, m_recv, c_send, c_recv,
):
    rows, cols, parts = sizes
    layers, d, k = w_hbm.shape
    rank = down_hbm.shape[1]
    half = 2 * rank
    full = EDGES * rank
    row, col, part = (lax.axis_index(a) for a in ("row", "col", "mp"))
    below = {"row": lax.rem(row + 1, rows)}
    above = {"row": lax.rem(row + rows - 1, rows)}
    right = {"col": lax.rem(col + 1, cols)}
    left = {"col": lax.rem(col + cols - 1, cols)}
    peers = [{"mp": lax.rem(part + i, parts)} for i in range(1, parts)]
    sides = (below, right, above, left)

    def load(l):
        return pltpu.make_async_copy(w_hbm.at[l], w.at[l], load_sem.at[l])

    def warm_loads():
        return [
            pltpu.make_async_copy(src, warm.at[i], warm_load.at[i])
            for i, src in enumerate((down_hbm, right_hbm))
        ]

    def remote(src, dst, send, recv, target):
        return pltpu.make_async_remote_copy(
            src_ref=src, dst_ref=dst, send_sem=send, recv_sem=recv,
            device_id=target, device_id_type=MESH,
        )

    def warm_copies():
        return [
            remote(warm.at[0], warm_in.at[0], warm_send.at[0], warm_recv.at[0], below),
            remote(warm.at[1], warm_in.at[1], warm_send.at[1], warm_recv.at[1], right),
        ]

    def m_copies(r, l, e):
        return [
            remote(
                ms.at[r, l, e], mr.at[r, l, i, e],
                m_send.at[i], m_recv.at[r, l, i, e], t,
            )
            for i, t in enumerate(peers)
        ]

    def edge_copy(src, dst, send, recv, r, l, e):
        o = (e + 2) % EDGES
        return remote(src.at[r, l, e], dst.at[r, l, o], send, recv.at[r, l, o], sides[e])

    def edge_wait(src, dst, send, recv, r, l, e):
        remote(
            src.at[r, l, e], dst.at[r, l, e], send, recv.at[r, l, e], sides[e]
        ).wait_recv()

    v_refs = (vs, vr, v_send, v_recv)
    c_refs = (cs, cr, c_send, c_recv)

    def each_layer(stage):
        def step(l, carry):
            stage(l)
            return carry
        lax.fori_loop(0, layers, step, 0)

    for copy in warm_loads():
        copy.start()
    each_layer(lambda l: load(l).start())
    barrier = pltpu.get_barrier_semaphore()
    partners = list(sides) + peers
    for t in partners:
        pl.semaphore_signal(barrier, inc=1, device_id=t, device_id_type=MESH)
    pl.semaphore_wait(barrier, len(partners))
    for copy in warm_loads():
        copy.wait()
    for copy in warm_copies():
        copy.start()

    width = piece(d, 768)

    def at_round(r):
        return slice(r * full, (r + 1) * full)

    def rows_of(e):
        return slice(e * rank, (e + 1) * rank)

    def launch(r, l, order, edges):
        for e in edges:
            if order == "sum":
                for copy in m_copies(r, l, e):
                    copy.start()
            else:
                edge_copy(*v_refs, r, l, e).start()

    def products(r, l, order, factors, edges, extra=None):
        out = ms if order == "sum" else vs
        cuts = [slice(at, at + width) for at in range(0, d, width)]
        parts = [
            lax.dot_general(
                factors, w[l, cut, :], (((1,), (1,)), ((), ())), preferred_element_type=F32
            )
            for cut in cuts
        ]
        for cut, f in zip(cuts, parts):
            if extra is not None:
                f = f + jnp.dot(extra, p_out[l, at_round(r - 1), cut], preferred_element_type=F32)
            first = edges[0] * rank
            kept[l, first : first + len(edges) * rank, cut] = f
            for i, e in enumerate(edges):
                out[r, l, e, :, cut] = f[rows_of(i)].astype(BF16)

    def own(r, l, e, order):
        load(l).wait()
        products(r, l, order, jnp.concatenate([warm[0, l], warm[1, l]], axis=0), (0, 1))
        launch(r, l, order, (0, 1))

    def far(r, l, e, order):
        if waiting:
            for copy in warm_copies():
                copy.wait_recv()
            waiting.clear()
        products(r, l, order, jnp.concatenate([warm_in[0, l], warm_in[1, l]], axis=0), (2, 3))
        launch(r, l, order, (2, 3))

    def forward(r, l, e, order):
        g = lax.dot_general(
            q[l], s_out[l, at_round(r - 1)], (((1,), (1,)), ((), ())), preferred_element_type=F32
        )
        products(r, l, order, q[l], (0, 1, 2, 3), g.astype(BF16))
        launch(r, l, order, (0, 2, 1, 3))

    def mid(r, l, e, order):
        here = rows_of(e)
        if order == "sum":
            for copy in m_copies(r, l, e):
                copy.wait_recv()
            v = kept[l, here]
            for i in range(len(peers)):
                v = v + mr[r, l, i, e].astype(F32)
            kept[l, here] = v
            vs[r, l, e] = v.astype(BF16)
            edge_copy(*v_refs, r, l, e).start()
        else:
            edge_wait(*v_refs, r, l, e)
            other = vr[r, l, e].astype(F32)
            v = kept[l, here] - other if e < 2 else other - kept[l, here]
            kept[l, here] = v
            ms[r, l, e] = v.astype(BF16)
            for copy in m_copies(r, l, e):
                copy.start()

    def basis(r, l, e, order):
        for i in range(EDGES):
            if order == "sum":
                edge_wait(*v_refs, r, l, i)
            else:
                for copy in m_copies(r, l, i):
                    copy.wait_recv()
        for h in range(2):
            pair = (2 * h, 2 * h + 1)
            v = kept[l, half * h : half * (h + 1)]
            if order == "sum":
                other = jnp.concatenate([vr[r, l, i].astype(F32) for i in pair], axis=0)
                v = v - other if h == 0 else other - v
            else:
                for j in range(len(peers)):
                    v = v + jnp.concatenate([mr[r, l, j, i].astype(F32) for i in pair], axis=0)
            at = r * full + half * h
            p_out[l, at : at + half] = orthonormal_pairs(v, rank).astype(BF16)
        b = jnp.dot(p_out[l, at_round(r)], w[l], preferred_element_type=F32)
        held[l] = b
        for i in range(EDGES):
            cs[r, l, i] = b[rows_of(i)].astype(BF16)
        for i in (0, 2, 1, 3):
            edge_copy(*c_refs, r, l, i).start()

    def combine(r, l, e, order):
        for i in range(EDGES):
            edge_wait(*c_refs, r, l, i)
        far_end = [
            jnp.concatenate([cr[r, l, i].astype(F32) for i in pair], axis=0)
            for pair in ((0, 1), (2, 3))
        ]
        mine = held[l, 0:half] - far_end[0]
        theirs = far_end[1] - held[l, half:full]
        if r == ROUNDS - 1:
            for i in range(2):
                c_out[i, l] = mine[rows_of(i)]
        else:
            q[l] = jnp.concatenate([mine, theirs], axis=0).astype(BF16)
        signed = jnp.concatenate([-mine, theirs], axis=0)
        s_out[l, at_round(r)] = (step_size * signed).astype(BF16)

    height = piece(d, 256)

    def update(r, l, e, order):
        before = at_round(r - 1)
        for at in range(0, d, height):
            cut = slice(at, at + height)
            change = lax.dot_general(
                p_out[l, before, cut], s_out[l, before], (((0,), (0,)), ((), ())),
                preferred_element_type=F32,
            )
            w[l, cut, :] = (w[l, cut, :].astype(F32) + change).astype(BF16)

    waiting = [True]
    stages = dict(own=own, far=far, forward=forward, mid=mid, basis=basis, combine=combine, update=update)
    for name, r, l, e, order in plan(layers):
        stages[name](r, l, e, order)

    for copy in warm_copies():
        copy.wait_send()

    for i, t in enumerate(peers):
        remote(ms, mr.at[:, :, i], m_send.at[i], m_recv.at[0, 0, i, 0], t).wait_send()
    remote(vs, vr, v_send, v_recv.at[0, 0, 0], below).wait_send()
    remote(cs, cr, c_send, c_recv.at[0, 0, 0], below).wait_send()


def gossip(sizes, layers, warm_down, warm_right):
    count, d, k = layers.shape
    rank = warm_down.shape[1]
    others = sizes[2] - 1
    full = EDGES * rank
    vmem = pl.BlockSpec(memory_space=pltpu.VMEM)
    hbm = pl.BlockSpec(memory_space=pltpu.HBM)
    dma = pltpu.SemaphoreType.DMA
    lead = (ROUNDS, count)
    return pl.pallas_call(
        functools.partial(gossip_kernel, sizes),
        out_shape=(
            jax.ShapeDtypeStruct((count, d, k), BF16),
            jax.ShapeDtypeStruct((count, ROUNDS * full, d), BF16),
            jax.ShapeDtypeStruct((count, ROUNDS * full, k), BF16),
            jax.ShapeDtypeStruct((2, count, rank, k), F32),
        ),
        in_specs=[hbm, hbm, hbm],
        out_specs=(vmem, vmem, vmem, vmem),
        scratch_shapes=[
            pltpu.VMEM((2, count, rank, k), BF16),
            pltpu.VMEM((2, count, rank, k), BF16),
            pltpu.VMEM((count, full, k), BF16),
            pltpu.VMEM((count, full, d), F32),
            pltpu.VMEM((count, full, k), F32),
            pltpu.VMEM(lead + (EDGES, rank, d), BF16),
            pltpu.VMEM(lead + (EDGES, rank, d), BF16),
            pltpu.VMEM(lead + (EDGES, rank, d), BF16),
            pltpu.VMEM(lead + (others, EDGES, rank, d), BF16),
            pltpu.VMEM(lead + (EDGES, rank, k), BF16),
            pltpu.VMEM(lead + (EDGES, rank, k), BF16),
            dma((count,)),
            dma((2,)),
            dma((2,)),
            dma((2,)),
            dma(()),
            dma(lead + (EDGES,)),
            dma((others,)),
            dma(lead + (others, EDGES)),
            dma(()),
            dma(lead + (EDGES,)),
        ],
        compiler_params=pltpu.CompilerParams(
            collective_id=0, has_side_effects=True, vmem_limit_bytes=40 * 2**20
        ),
    )(layers, warm_down, warm_right)


def finish_kernel(w, p, s, c, out, down, right, held, out_sem, c_sem):
    layers, d, k = w.shape
    height = piece(d, 256)
    block = piece(d, 768)
    full = p.shape[1] // ROUNDS
    last = slice((ROUNDS - 1) * full, ROUNDS * full)
    small = [
        pltpu.make_async_copy(c.at[i], dst, c_sem.at[i]) for i, dst in enumerate((down, right))
    ]
    for copy in small:
        copy.start()

    def store(l, b):
        span = pl.ds(b * block, block)
        return pltpu.make_async_copy(held.at[l, span], out.at[l, span], out_sem.at[l, b])

    for l in range(layers):
        for b in range(d // block):
            for at in range(b * block, (b + 1) * block, height):
                cut = slice(at, at + height)
                change = lax.dot_general(
                    p[l, last, cut], s[l, last], (((0,), (0,)), ((), ())),
                    preferred_element_type=F32,
                )
                held[l, cut, :] = (w[l, cut, :].astype(F32) + change).astype(BF16)
            store(l, b).start()
    for copy in small:
        copy.wait()
    for l in range(layers):
        for b in range(d // block):
            store(l, b).wait()


def last_update(w0, basis, factors, combined):
    count, d, k = w0.shape
    rank = combined.shape[2]
    vmem = pl.BlockSpec(memory_space=pltpu.VMEM)
    hbm = pl.BlockSpec(memory_space=pltpu.HBM)
    dma = pltpu.SemaphoreType.DMA
    return pl.pallas_call(
        finish_kernel,
        out_shape=(
            jax.ShapeDtypeStruct((count, d, k), BF16),
            jax.ShapeDtypeStruct((count, rank, k), F32),
            jax.ShapeDtypeStruct((count, rank, k), F32),
        ),
        in_specs=[vmem, vmem, vmem, vmem],
        out_specs=(hbm, hbm, hbm),
        scratch_shapes=[
            pltpu.VMEM((count, d, k), BF16),
            dma((count, d // piece(d, 768))),
            dma((2,)),
        ],
        compiler_params=pltpu.CompilerParams(vmem_limit_bytes=24 * 2**20),
    )(w0, basis, factors, combined)


def solution(mesh):
    sizes = tuple(mesh.shape[a] for a in ("row", "col", "mp"))

    def body(weights, warm_down, warm_right):
        parts = gossip(sizes, weights[0, 0], warm_down[0, 0], warm_right[0, 0])
        new, down, right = last_update(*parts)
        return new[None, None], down[None, None], right[None, None]

    spec = P("row", "col", None, None, "mp")
    return jax.shard_map(
        body, mesh=mesh, in_specs=(spec,) * 3, out_specs=(spec,) * 3, check_vma=False
    )
```

```python
import functools

import jax
import jax.numpy as jnp
from jax import lax
from jax.experimental import pallas as pl
from jax.experimental.pallas import tpu as pltpu
from jax.sharding import PartitionSpec as P

ROUNDS = 2

step_size = 0.2
epsilon = 1e-06

MESH = pl.DeviceIdType.MESH
F32 = jnp.float32
BF16 = jnp.bfloat16
EDGES = 4


def piece(total, want):
    size = min(total, want)
    while total % size:
        size -= 128
    return size


def total(values):
    return functools.reduce(lambda a, b: a + b, values)


def orthonormal_pairs(v, rank):
    row = lax.broadcasted_iota(jnp.int32, (v.shape[0], 1), 0)
    first = row < rank
    within = jnp.where(first, row, row - rank)
    turned = [v] + [pltpu.roll(v, s, 0) for s in range(1, rank)]
    inner = [jnp.sum(v * t, axis=-1, keepdims=True) for t in turned]

    def pick(k, j):
        k, j = max(k, j), min(k, j)
        dots = inner[k - j]
        return jnp.where(first, dots[k : k + 1], dots[rank + k : rank + k + 1])

    gram = [[pick(k, j) for j in range(rank)] for k in range(rank)]
    mix, inverse = [], []
    for k in range(rank):
        ahead = [
            total([mix[j][i] * gram[k][i] for i in range(j)] + [gram[k][j]])
            * (inverse[j] * inverse[j])
            for j in range(k)
        ]
        mix.append([
            -total([ahead[j] * mix[j][i] for j in range(i + 1, k)] + [ahead[i]])
            for i in range(k)
        ])
        along = [
            total([mix[k][i] * gram[i][j] for i in range(k)] + [gram[k][j]])
            for j in range(k + 1)
        ]
        norm = total([mix[k][j] * along[j] for j in range(k)] + [along[k]])
        inverse.append(lax.rsqrt(jnp.maximum(norm, 0.0) + epsilon))
    out = None
    for s in range(rank):
        weight = jnp.zeros(row.shape, F32)
        for k in range(s, rank):
            entry = inverse[k] if s == 0 else inverse[k] * mix[k][k - s]
            weight = jnp.where(within == k, entry, weight)
        out = weight * turned[s] if s == 0 else out + weight * turned[s]
    return out


COST = {
    "own": 0.85, "far": 0.5, "forward": 0.7, "mid": 0.04, "basis": 0.62, "combine": 0.14,
    "update": 0.8,
}
ROW, COL, PART, ACROSS, ALONG, SKEW = 3.4, 2.4, 2.5, 0.4, 0.4, 0.5
ENDS = {1: 2}
EARLY = 2
RANKED = ("mid", "combine", "basis", "forward", "far", "own", "update")


def groups(r):
    return ((0, 1), (2, 3)) if r == 0 else ((0, 2), (1, 3))


def plan(layers):
    def order(r, l):
        return "ends" if l >= layers - ENDS.get(r, 0) else "sum"

    wires = {}
    now, done = 0.0, []
    ready = {("own", 0, l, 0): 2.2 + 0.4 * l for l in range(layers)}
    ready.update({("far", 0, l, 0): 6.0 for l in range(layers)})
    arrived = {}

    def over(wire, t, size, latency):
        wires[wire] = max(wires.get(wire, 0.0), t) + size
        return wires[wire] + latency

    def hop(e, t):
        return over(("row", e), t, ALONG, ROW) if e % 2 == 0 else t + COL

    def across(t):
        return over("mp", t, ACROSS, PART)

    def sent(r, l, which, t):
        for g in which:
            ready["mid", r, l, g] = max(
                across(t) if order(r, l) == "sum" else hop(e, t) for e in groups(r)[g]
            )
            if r == 0 and g == 0:
                ready["mid", r, l, g] += SKEW

    while ready:
        soon = [k for k, t in ready.items() if t <= now]
        if soon:
            key = min(soon, key=lambda k: (RANKED.index(k[0]), ready[k], k))
        else:
            key = min(ready, key=lambda k: (ready[k], k))
        name, r, l, g = key
        now = max(now, ready.pop(key)) + COST[name]
        done.append(key)
        if name == "own":
            sent(r, l, (0,), now)
        elif name == "far":
            sent(r, l, (1,), now)
        elif name == "forward":
            sent(r, l, (0, 1), now)
            ready["update", r, l, 0] = now
        elif name == "mid":
            got = arrived.setdefault((r, l), [])
            for e in groups(r)[g]:
                got.append(hop(e, now) if order(r, l) == "sum" else across(now))
        elif name == "basis":
            ready["combine", r, l, 0] = now + ROW + 0.2
        elif name == "combine" and r + 1 < ROUNDS:
            ready["forward", r + 1, l, 0] = now
        elif name == "combine" and l < EARLY:
            ready["update", r + 1, l, 0] = now
        if len(arrived.get((r, l), ())) == EDGES and (r == 0 or ("update", r, l, 0) in done):
            if ("basis", r, l, 0) not in done:
                ready["basis", r, l, 0] = max(arrived[r, l])
    return [(name, r, l, g, order(r, l)) for name, r, l, g in done]


def gossip_kernel(
    sizes, w_hbm, down_hbm, right_hbm, w, p_out, s_out, c_out,
    warm, warm_in, turned, q, cross, kept, held, vs, vr, ms, mr, cs, cr,
    load_sem, warm_load, warm_send, warm_recv, v_send, v_recv,
    m_send, m_recv, c_send, c_recv,
):
    rows, cols, parts = sizes
    layers, d, k = w_hbm.shape
    rank = down_hbm.shape[1]
    half = 2 * rank
    full = EDGES * rank
    row, col, part = (lax.axis_index(a) for a in ("row", "col", "mp"))
    below = {"row": lax.rem(row + 1, rows)}
    above = {"row": lax.rem(row + rows - 1, rows)}
    right = {"col": lax.rem(col + 1, cols)}
    left = {"col": lax.rem(col + cols - 1, cols)}
    peers = [{"mp": lax.rem(part + i, parts)} for i in range(1, parts)]
    sides = (below, right, above, left)

    def load(l):
        return pltpu.make_async_copy(w_hbm.at[l], w.at[l], load_sem.at[l])

    def warm_loads():
        return [
            pltpu.make_async_copy(src, warm.at[i], warm_load)
            for i, src in enumerate((down_hbm, right_hbm))
        ]

    def remote(src, dst, send, recv, target):
        return pltpu.make_async_remote_copy(
            src_ref=src, dst_ref=dst, send_sem=send, recv_sem=recv,
            device_id=target, device_id_type=MESH,
        )

    def warm_copies():
        return [
            remote(warm.at[0], warm_in.at[0], warm_send, warm_recv, below),
            remote(warm.at[1], warm_in.at[1], warm_send, warm_recv, right),
        ]

    def group(r, e):
        return [e in g for g in groups(r)].index(True)

    def m_copies(r, l, e):
        return [
            remote(ms.at[r, l, e], mr.at[r, l, i, e], m_send.at[i], m_recv.at[r, l, i, group(r, e)], t)
            for i, t in enumerate(peers)
        ]

    def v_copy(r, l, e):
        o = (e + 2) % EDGES
        return remote(vs.at[r, l, e], vr.at[r, l, o], v_send, v_recv.at[l, group(r, o)], sides[e])

    def c_copy(r, l, e):
        return remote(cs.at[r, l, e], cr.at[r, l, (e + 2) % EDGES], c_send, c_recv.at[l], sides[e])

    def m_arrive(r, l, g):
        for i, t in enumerate(peers):
            remote(
                ms.at[r, l, 0:2], mr.at[r, l, i, 0:2], m_send.at[i], m_recv.at[r, l, i, g], t
            ).wait_recv()

    def v_arrive(r, l, g):
        remote(vs.at[r, l, 0:2], vr.at[r, l, 0:2], v_send, v_recv.at[l, g], below).wait_recv()

    def c_arrive(r, l):
        remote(cs.at[r, l], cr.at[r, l], c_send, c_recv.at[l], below).wait_recv()

    def each_layer(stage):
        def step(l, carry):
            stage(l)
            return carry
        lax.fori_loop(0, layers, step, 0)

    for copy in warm_loads():
        copy.start()
    each_layer(lambda l: load(l).start())
    barrier = pltpu.get_barrier_semaphore()
    partners = list(sides) + peers
    for t in partners:
        pl.semaphore_signal(barrier, inc=1, device_id=t, device_id_type=MESH)
    pl.semaphore_wait(barrier, len(partners))
    pltpu.make_async_copy(warm, warm_in, warm_load).wait()
    for copy in warm_copies():
        copy.start()

    width = piece(d, 768)

    def at_round(r):
        return slice(r * full, (r + 1) * full)

    def rows_of(e):
        return slice(e * rank, (e + 1) * rank)

    def launch(r, l, order, edges):
        for e in edges:
            if order == "sum":
                for copy in m_copies(r, l, e):
                    copy.start()
            else:
                v_copy(r, l, e).start()

    def products(r, l, order, factors, edges, extra=None):
        out = ms if order == "sum" else vs
        cuts = [slice(at, at + width) for at in range(0, d, width)]
        parts = []
        for cut in cuts:
            if edges == (0, 1):
                turned[l, :, cut] = w[l, cut, :].T
            parts.append(jnp.dot(factors, turned[l, :, cut], preferred_element_type=F32))
        for cut, f in zip(cuts, parts):
            if extra is not None:
                f = f + jnp.dot(extra, p_out[l, at_round(r - 1), cut], preferred_element_type=F32)
            first = edges[0] * rank
            kept[l, first : first + len(edges) * rank, cut] = f
            for i, e in enumerate(edges):
                out[r, l, e, :, cut] = f[rows_of(i)].astype(BF16)

    def own(r, l, e, order):
        load(l).wait()
        products(r, l, order, jnp.concatenate([warm[0, l], warm[1, l]], axis=0), (0, 1))
        launch(r, l, order, (0, 1))

    def far(r, l, e, order):
        if waiting:
            remote(warm, warm_in, warm_send, warm_recv, below).wait_recv()
            waiting.clear()
        products(r, l, order, jnp.concatenate([warm_in[0, l], warm_in[1, l]], axis=0), (2, 3))
        launch(r, l, order, (2, 3))

    def forward(r, l, e, order):
        products(r, l, order, q[l], (0, 1, 2, 3), cross[l])
        launch(r, l, order, (0, 2, 1, 3))

    def mid(r, l, g, order):
        if order == "sum":
            m_arrive(r, l, g)
        else:
            v_arrive(r, l, g)
        for e in groups(r)[g]:
            here = rows_of(e)
            v = kept[l, here]
            if order == "sum":
                for i in range(len(peers)):
                    v = v + mr[r, l, i, e].astype(F32)
            else:
                other = vr[r, l, e].astype(F32)
                v = v - other if e < 2 else other - v
            kept[l, here] = v
            out = vs if order == "sum" else ms
            out[r, l, e] = v.astype(BF16)
        for e in groups(r)[g]:
            if order == "sum":
                v_copy(r, l, e).start()
            else:
                for copy in m_copies(r, l, e):
                    copy.start()

    def basis(r, l, e, order):
        for g in range(2):
            if order == "sum":
                v_arrive(r, l, g)
            else:
                m_arrive(r, l, g)
        for h in range(2):
            pair = (2 * h, 2 * h + 1)
            v = kept[l, half * h : half * (h + 1)]
            if order == "sum":
                other = jnp.concatenate([vr[r, l, i].astype(F32) for i in pair], axis=0)
                v = v - other if h == 0 else other - v
            else:
                for j in range(len(peers)):
                    v = v + jnp.concatenate([mr[r, l, j, i].astype(F32) for i in pair], axis=0)
            at = r * full + half * h
            p_out[l, at : at + half] = orthonormal_pairs(v, rank).astype(BF16)
        b = jnp.dot(p_out[l, at_round(r)], w[l], preferred_element_type=F32)
        held[l] = b
        for i in range(EDGES):
            cs[r, l, i] = b[rows_of(i)].astype(BF16)
        for i in (0, 2, 1, 3):
            c_copy(r, l, i).start()

    def combine(r, l, e, order):
        c_arrive(r, l)
        far_end = [
            jnp.concatenate([cr[r, l, i].astype(F32) for i in pair], axis=0)
            for pair in ((0, 1), (2, 3))
        ]
        mine = held[l, 0:half] - far_end[0]
        theirs = far_end[1] - held[l, half:full]
        signed = (step_size * jnp.concatenate([-mine, theirs], axis=0)).astype(BF16)
        s_out[l, at_round(r)] = signed
        if r == ROUNDS - 1:
            for i in range(2):
                c_out[i, l] = mine[rows_of(i)]
        else:
            factors = jnp.concatenate([mine, theirs], axis=0).astype(BF16)
            q[l] = factors
            cross[l] = lax.dot_general(
                factors, signed, (((1,), (1,)), ((), ())), preferred_element_type=F32
            ).astype(BF16)

    height = piece(d, 256)

    def update(r, l, e, order):
        before = at_round(r - 1)
        for at in range(0, d, height):
            cut = slice(at, at + height)
            change = lax.dot_general(
                p_out[l, before, cut], s_out[l, before], (((0,), (0,)), ((), ())),
                preferred_element_type=F32,
            )
            w[l, cut, :] = (w[l, cut, :].astype(F32) + change).astype(BF16)

    waiting = [True]
    stages = dict(own=own, far=far, forward=forward, mid=mid, basis=basis, combine=combine, update=update)
    for name, r, l, e, order in plan(layers):
        stages[name](r, l, e, order)

    remote(warm, warm_in, warm_send, warm_recv, below).wait_send()

    for i, t in enumerate(peers):
        remote(ms, mr.at[:, :, i], m_send.at[i], m_recv.at[0, 0, i, 0], t).wait_send()
    remote(vs, vr, v_send, v_recv.at[0, 0], below).wait_send()
    remote(cs, cr, c_send, c_recv.at[0], below).wait_send()


def gossip(sizes, layers, warm_down, warm_right):
    count, d, k = layers.shape
    rank = warm_down.shape[1]
    others = sizes[2] - 1
    full = EDGES * rank
    vmem = pl.BlockSpec(memory_space=pltpu.VMEM)
    hbm = pl.BlockSpec(memory_space=pltpu.HBM)
    dma = pltpu.SemaphoreType.DMA
    lead = (ROUNDS, count)
    return pl.pallas_call(
        functools.partial(gossip_kernel, sizes),
        out_shape=(
            jax.ShapeDtypeStruct((count, d, k), BF16),
            jax.ShapeDtypeStruct((count, ROUNDS * full, d), BF16),
            jax.ShapeDtypeStruct((count, ROUNDS * full, k), BF16),
            jax.ShapeDtypeStruct((2, count, rank, k), F32),
        ),
        in_specs=[hbm, hbm, hbm],
        out_specs=(vmem, vmem, vmem, vmem),
        scratch_shapes=[
            pltpu.VMEM((2, count, rank, k), BF16),
            pltpu.VMEM((2, count, rank, k), BF16),
            pltpu.VMEM((count, k, d), BF16),
            pltpu.VMEM((count, full, k), BF16),
            pltpu.VMEM((count, full, full), BF16),
            pltpu.VMEM((count, full, d), F32),
            pltpu.VMEM((count, full, k), F32),
            pltpu.VMEM(lead + (EDGES, rank, d), BF16),
            pltpu.VMEM(lead + (EDGES, rank, d), BF16),
            pltpu.VMEM(lead + (EDGES, rank, d), BF16),
            pltpu.VMEM(lead + (others, EDGES, rank, d), BF16),
            pltpu.VMEM(lead + (EDGES, rank, k), BF16),
            pltpu.VMEM(lead + (EDGES, rank, k), BF16),
            dma((count,)),
            dma(()),
            dma(()),
            dma(()),
            dma(()),
            dma((count, 2)),
            dma((others,)),
            dma(lead + (others, 2)),
            dma(()),
            dma((count,)),
        ],
        compiler_params=pltpu.CompilerParams(
            collective_id=0, has_side_effects=True, vmem_limit_bytes=40 * 2**20
        ),
    )(layers, warm_down, warm_right)


def finish_kernel(w, p, s, c, out, down, right, held, out_sem, c_sem):
    layers, d, k = w.shape
    height = piece(d, 256)
    block = piece(d, 768)
    full = p.shape[1] // ROUNDS
    last = slice((ROUNDS - 1) * full, ROUNDS * full)
    small = [
        pltpu.make_async_copy(c.at[i], dst, c_sem.at[i]) for i, dst in enumerate((down, right))
    ]
    for copy in small:
        copy.start()

    def store(l, b):
        span = pl.ds(b * block, block)
        source = w if l < EARLY else held
        return pltpu.make_async_copy(source.at[l, span], out.at[l, span], out_sem.at[l, b])

    blocks = [(l, b) for l in range(layers) for b in range(d // block)]
    for l, b in blocks:
        if l >= EARLY:
            for at in range(b * block, (b + 1) * block, height):
                cut = slice(at, at + height)
                change = lax.dot_general(
                    p[l, last, cut], s[l, last], (((0,), (0,)), ((), ())),
                    preferred_element_type=F32,
                )
                held[l, cut, :] = (w[l, cut, :].astype(F32) + change).astype(BF16)
        store(l, b).start()
    for copy in small:
        copy.wait()
    for l, b in blocks:
        store(l, b).wait()


def last_update(w0, basis, factors, combined):
    count, d, k = w0.shape
    rank = combined.shape[2]
    vmem = pl.BlockSpec(memory_space=pltpu.VMEM)
    hbm = pl.BlockSpec(memory_space=pltpu.HBM)
    dma = pltpu.SemaphoreType.DMA
    return pl.pallas_call(
        finish_kernel,
        out_shape=(
            jax.ShapeDtypeStruct((count, d, k), BF16),
            jax.ShapeDtypeStruct((count, rank, k), F32),
            jax.ShapeDtypeStruct((count, rank, k), F32),
        ),
        in_specs=[vmem, vmem, vmem, vmem],
        out_specs=(hbm, hbm, hbm),
        scratch_shapes=[
            pltpu.VMEM((count, d, k), BF16),
            dma((count, d // piece(d, 768))),
            dma((2,)),
        ],
        compiler_params=pltpu.CompilerParams(vmem_limit_bytes=24 * 2**20),
    )(w0, basis, factors, combined)


def solution(mesh):
    sizes = tuple(mesh.shape[a] for a in ("row", "col", "mp"))

    def body(weights, warm_down, warm_right):
        warm = [
            pltpu.with_memory_space_constraint(x[0, 0], pltpu.HBM)
            for x in (warm_down, warm_right)
        ]
        parts = gossip(sizes, weights[0, 0], *warm)
        new, down, right = last_update(*parts)
        return new[None, None], down[None, None], right[None, None]

    spec = P("row", "col", None, None, "mp")
    return jax.shard_map(
        body, mesh=mesh, in_specs=(spec,) * 3, out_specs=(spec,) * 3, check_vma=False
    )
```

```python
import functools

import jax
import jax.numpy as jnp
from jax import lax
from jax.experimental import pallas as pl
from jax.experimental.pallas import tpu as pltpu
from jax.sharding import PartitionSpec as P

ROUNDS = 2

step_size = 0.2
epsilon = 1e-06

MESH = pl.DeviceIdType.MESH
F32 = jnp.float32
BF16 = jnp.bfloat16
EDGES = 4


def piece(total, want):
    size = min(total, want)
    while total % size:
        size -= 128
    return size


def total(values):
    return functools.reduce(lambda a, b: a + b, values)


def orthonormal_pairs(v, rank):
    row = lax.broadcasted_iota(jnp.int32, (v.shape[0], 1), 0)
    first = row < rank
    within = jnp.where(first, row, row - rank)
    turned = [v] + [pltpu.roll(v, s, 0) for s in range(1, rank)]
    inner = [jnp.sum(v * t, axis=-1, keepdims=True) for t in turned]

    def pick(k, j):
        k, j = max(k, j), min(k, j)
        dots = inner[k - j]
        return jnp.where(first, dots[k : k + 1], dots[rank + k : rank + k + 1])

    gram = [[pick(k, j) for j in range(rank)] for k in range(rank)]
    mix, inverse = [], []
    for k in range(rank):
        ahead = [
            total([mix[j][i] * gram[k][i] for i in range(j)] + [gram[k][j]])
            * (inverse[j] * inverse[j])
            for j in range(k)
        ]
        mix.append([
            -total([ahead[j] * mix[j][i] for j in range(i + 1, k)] + [ahead[i]])
            for i in range(k)
        ])
        along = [
            total([mix[k][i] * gram[i][j] for i in range(k)] + [gram[k][j]])
            for j in range(k + 1)
        ]
        norm = total([mix[k][j] * along[j] for j in range(k)] + [along[k]])
        inverse.append(lax.rsqrt(jnp.maximum(norm, 0.0) + epsilon))
    out = None
    for s in range(rank):
        weight = jnp.zeros(row.shape, F32)
        for k in range(s, rank):
            entry = inverse[k] if s == 0 else inverse[k] * mix[k][k - s]
            weight = jnp.where(within == k, entry, weight)
        out = weight * turned[s] if s == 0 else out + weight * turned[s]
    return out


COST = {
    "own": 0.85, "far": 0.5, "forward": 0.7, "mid": 0.04, "basis": 0.62, "combine": 0.14,
    "update": 0.8,
}
ROW, COL, PART, ACROSS, ALONG, SKEW = 3.4, 2.4, 2.5, 0.4, 0.4, 0.5
ENDS = {0: 2, 1: 2}
EARLY = 2
START, WARM, LATE = 1.0, 5.0, 2.0
RANKED = ("mid", "combine", "basis", "forward", "far", "own", "update")


def groups(r):
    return ((0, 1), (2, 3)) if r == 0 else ((0, 2), (1, 3))


def plan(layers):
    def order(r, l):
        return "ends" if l >= layers - ENDS.get(r, 0) else "sum"

    wires = {}
    now, done = 0.0, []
    ready = {("own", 0, l, 0): START + 0.3 * l for l in range(layers)}
    arrived, early = {}, {}

    def over(wire, t, size, latency):
        wires[wire] = max(wires.get(wire, 0.0), t) + size
        return wires[wire] + latency

    def hop(e, t):
        return over(("row", e), t, ALONG, ROW) if e % 2 == 0 else t + COL

    def across(t):
        return over("mp", t, ACROSS, PART)

    def sent(r, l, which, t):
        for g in which:
            ready["mid", r, l, g] = max(
                across(t) if order(r, l) == "sum" else hop(e, t) for e in groups(r)[g]
            )
            if name == "own":
                ready["mid", r, l, g] += SKEW

    while ready:
        soon = [k for k, t in ready.items() if t <= now]
        if soon:
            key = min(soon, key=lambda k: (RANKED.index(k[0]), ready[k], k))
        else:
            key = min(ready, key=lambda k: (ready[k], k))
        name, r, l, g = key
        now = max(now, ready.pop(key)) + COST[name]
        done.append(key)
        if name == "own":
            ready["far", r, l, 0] = max(now, WARM)
            if order(r, l) == "sum":
                sent(r, l, (0,), now)
            else:
                early[l] = max(hop(e, now) for e in groups(r)[0]) + LATE
        elif name == "far" and order(r, l) == "sum":
            sent(r, l, (1,), now)
        elif name == "far":
            ready["mid", r, l, 1] = max(now, early[l])
            ready["mid", r, l, 0] = max(hop(e, now) for e in groups(r)[1])
        elif name == "forward":
            sent(r, l, (0, 1), now)
            ready["update", r, l, 0] = now
        elif name == "mid":
            got = arrived.setdefault((r, l), [])
            for e in groups(r)[g]:
                got.append(hop(e, now) if order(r, l) == "sum" else across(now))
        elif name == "basis":
            ready["combine", r, l, 0] = now + ROW + 0.2
        elif name == "combine" and r + 1 < ROUNDS:
            ready["forward", r + 1, l, 0] = now
        elif name == "combine" and l < EARLY:
            ready["update", r + 1, l, 0] = now
        if len(arrived.get((r, l), ())) == EDGES and (r == 0 or ("update", r, l, 0) in done):
            if ("basis", r, l, 0) not in done:
                ready["basis", r, l, 0] = max(arrived[r, l])
    return [(name, r, l, g, order(r, l)) for name, r, l, g in done]


def gossip_kernel(
    sizes, w_hbm, down_hbm, right_hbm, w, p_out, s_out, c_out,
    warm, warm_in, turned, q, cross, kept, held, vs, vr, ms, mr, cs, cr,
    load_sem, warm_load, warm_send, warm_recv, v_send, v_recv,
    m_send, m_recv, c_send, c_recv,
):
    rows, cols, parts = sizes
    layers, d, k = w_hbm.shape
    rank = down_hbm.shape[1]
    half = 2 * rank
    full = EDGES * rank
    row, col, part = (lax.axis_index(a) for a in ("row", "col", "mp"))
    below = {"row": lax.rem(row + 1, rows)}
    above = {"row": lax.rem(row + rows - 1, rows)}
    right = {"col": lax.rem(col + 1, cols)}
    left = {"col": lax.rem(col + cols - 1, cols)}
    peers = [{"mp": lax.rem(part + i, parts)} for i in range(1, parts)]
    sides = (below, right, above, left)

    def load(l):
        return pltpu.make_async_copy(w_hbm.at[l], w.at[l], load_sem.at[l])

    def warm_loads():
        return [
            pltpu.make_async_copy(src, warm.at[i], warm_load)
            for i, src in enumerate((down_hbm, right_hbm))
        ]

    def remote(src, dst, send, recv, target):
        return pltpu.make_async_remote_copy(
            src_ref=src, dst_ref=dst, send_sem=send, recv_sem=recv,
            device_id=target, device_id_type=MESH,
        )

    def warm_copies():
        return [
            remote(warm.at[0], warm_in.at[0], warm_send, warm_recv, below),
            remote(warm.at[1], warm_in.at[1], warm_send, warm_recv, right),
        ]

    def group(r, e):
        return [e in g for g in groups(r)].index(True)

    def m_copies(r, l, e):
        return [
            remote(ms.at[r, l, e], mr.at[r, l, i, e], m_send.at[i], m_recv.at[r, l, i, group(r, e)], t)
            for i, t in enumerate(peers)
        ]

    def v_copy(r, l, e):
        o = (e + 2) % EDGES
        return remote(vs.at[r, l, e], vr.at[r, l, o], v_send, v_recv.at[l, group(r, o)], sides[e])

    def c_copy(r, l, e):
        return remote(cs.at[r, l, e], cr.at[r, l, (e + 2) % EDGES], c_send, c_recv.at[l], sides[e])

    def m_arrive(r, l, g):
        for i, t in enumerate(peers):
            remote(
                ms.at[r, l, 0:2], mr.at[r, l, i, 0:2], m_send.at[i], m_recv.at[r, l, i, g], t
            ).wait_recv()

    def v_arrive(r, l, g):
        remote(vs.at[r, l, 0:2], vr.at[r, l, 0:2], v_send, v_recv.at[l, g], below).wait_recv()

    def c_arrive(r, l):
        remote(cs.at[r, l], cr.at[r, l], c_send, c_recv.at[l], below).wait_recv()

    def each_layer(stage):
        def step(l, carry):
            stage(l)
            return carry
        lax.fori_loop(0, layers, step, 0)

    for copy in warm_loads():
        copy.start()
    each_layer(lambda l: load(l).start())
    barrier = pltpu.get_barrier_semaphore()
    partners = list(sides) + peers
    for t in partners:
        pl.semaphore_signal(barrier, inc=1, device_id=t, device_id_type=MESH)
    width = piece(d, 768)

    def at_round(r):
        return slice(r * full, (r + 1) * full)

    def rows_of(e):
        return slice(e * rank, (e + 1) * rank)

    def launch(r, l, order, edges):
        for e in edges:
            if order == "sum":
                for copy in m_copies(r, l, e):
                    copy.start()
            else:
                v_copy(r, l, e).start()

    def products(r, l, order, factors, edges, extra=None):
        out = ms if order == "sum" else vs
        cuts = [slice(at, at + width) for at in range(0, d, width)]
        parts = []
        for cut in cuts:
            if edges == (0, 1):
                turned[l, :, cut] = w[l, cut, :].T
            parts.append(jnp.dot(factors, turned[l, :, cut], preferred_element_type=F32))
        for cut, f in zip(cuts, parts):
            if extra is not None:
                f = f + jnp.dot(extra, p_out[l, at_round(r - 1), cut], preferred_element_type=F32)
            first = edges[0] * rank
            kept[l, first : first + len(edges) * rank, cut] = f
            for i, e in enumerate(edges):
                out[r, l, e, :, cut] = f[rows_of(i)].astype(BF16)

    def own(r, l, e, order):
        load(l).wait()
        products(r, l, order, jnp.concatenate([warm[0, l], warm[1, l]], axis=0), (0, 1))
        launch(r, l, order, (0, 1))

    def far(r, l, e, order):
        if waiting:
            remote(warm, warm_in, warm_send, warm_recv, below).wait_recv()
            waiting.clear()
        products(r, l, order, jnp.concatenate([warm_in[0, l], warm_in[1, l]], axis=0), (2, 3))
        launch(r, l, order, (2, 3))

    def forward(r, l, e, order):
        products(r, l, order, q[l], (0, 1, 2, 3), cross[l])
        launch(r, l, order, (0, 2, 1, 3))

    def mid(r, l, g, order):
        if order == "sum":
            m_arrive(r, l, g)
        else:
            v_arrive(r, l, g)
        for e in groups(r)[g]:
            here = rows_of(e)
            v = kept[l, here]
            if order == "sum":
                for i in range(len(peers)):
                    v = v + mr[r, l, i, e].astype(F32)
            else:
                other = vr[r, l, e].astype(F32)
                v = v - other if e < 2 else other - v
            kept[l, here] = v
            out = vs if order == "sum" else ms
            out[r, l, e] = v.astype(BF16)
        for e in groups(r)[g]:
            if order == "sum":
                v_copy(r, l, e).start()
            else:
                for copy in m_copies(r, l, e):
                    copy.start()

    def basis(r, l, e, order):
        for g in range(2):
            if order == "sum":
                v_arrive(r, l, g)
            else:
                m_arrive(r, l, g)
        for h in range(2):
            pair = (2 * h, 2 * h + 1)
            v = kept[l, half * h : half * (h + 1)]
            if order == "sum":
                other = jnp.concatenate([vr[r, l, i].astype(F32) for i in pair], axis=0)
                v = v - other if h == 0 else other - v
            else:
                for j in range(len(peers)):
                    v = v + jnp.concatenate([mr[r, l, j, i].astype(F32) for i in pair], axis=0)
            at = r * full + half * h
            p_out[l, at : at + half] = orthonormal_pairs(v, rank).astype(BF16)
        b = jnp.dot(p_out[l, at_round(r)], w[l], preferred_element_type=F32)
        held[l] = b
        for i in range(EDGES):
            cs[r, l, i] = b[rows_of(i)].astype(BF16)
        for i in (0, 2, 1, 3):
            c_copy(r, l, i).start()

    def combine(r, l, e, order):
        c_arrive(r, l)
        far_end = [
            jnp.concatenate([cr[r, l, i].astype(F32) for i in pair], axis=0)
            for pair in ((0, 1), (2, 3))
        ]
        mine = held[l, 0:half] - far_end[0]
        theirs = far_end[1] - held[l, half:full]
        signed = (step_size * jnp.concatenate([-mine, theirs], axis=0)).astype(BF16)
        s_out[l, at_round(r)] = signed
        if r == ROUNDS - 1:
            for i in range(2):
                c_out[i, l] = mine[rows_of(i)]
        else:
            factors = jnp.concatenate([mine, theirs], axis=0).astype(BF16)
            q[l] = factors
            cross[l] = lax.dot_general(
                factors, signed, (((1,), (1,)), ((), ())), preferred_element_type=F32
            ).astype(BF16)

    height = piece(d, 256)

    def update(r, l, e, order):
        before = at_round(r - 1)
        for at in range(0, d, height):
            cut = slice(at, at + height)
            change = lax.dot_general(
                p_out[l, before, cut], s_out[l, before], (((0,), (0,)), ((), ())),
                preferred_element_type=F32,
            )
            w[l, cut, :] = (w[l, cut, :].astype(F32) + change).astype(BF16)

    waiting = [True]
    pltpu.make_async_copy(warm, warm_in, warm_load).wait()
    pl.semaphore_wait(barrier, len(partners))
    for copy in warm_copies():
        copy.start()
    stages = dict(own=own, far=far, forward=forward, mid=mid, basis=basis, combine=combine, update=update)
    for name, r, l, e, order in plan(layers):
        stages[name](r, l, e, order)

    remote(warm, warm_in, warm_send, warm_recv, below).wait_send()

    for i, t in enumerate(peers):
        remote(ms, mr.at[:, :, i], m_send.at[i], m_recv.at[0, 0, i, 0], t).wait_send()
    remote(vs, vr, v_send, v_recv.at[0, 0], below).wait_send()
    remote(cs, cr, c_send, c_recv.at[0], below).wait_send()


def gossip(sizes, layers, warm_down, warm_right):
    count, d, k = layers.shape
    rank = warm_down.shape[1]
    others = sizes[2] - 1
    full = EDGES * rank
    vmem = pl.BlockSpec(memory_space=pltpu.VMEM)
    hbm = pl.BlockSpec(memory_space=pltpu.HBM)
    dma = pltpu.SemaphoreType.DMA
    lead = (ROUNDS, count)
    return pl.pallas_call(
        functools.partial(gossip_kernel, sizes),
        out_shape=(
            jax.ShapeDtypeStruct((count, d, k), BF16),
            jax.ShapeDtypeStruct((count, ROUNDS * full, d), BF16),
            jax.ShapeDtypeStruct((count, ROUNDS * full, k), BF16),
            jax.ShapeDtypeStruct((2, count, rank, k), F32),
        ),
        in_specs=[hbm, hbm, hbm],
        out_specs=(vmem, vmem, vmem, vmem),
        scratch_shapes=[
            pltpu.VMEM((2, count, rank, k), BF16),
            pltpu.VMEM((2, count, rank, k), BF16),
            pltpu.VMEM((count, k, d), BF16),
            pltpu.VMEM((count, full, k), BF16),
            pltpu.VMEM((count, full, full), BF16),
            pltpu.VMEM((count, full, d), F32),
            pltpu.VMEM((count, full, k), F32),
            pltpu.VMEM(lead + (EDGES, rank, d), BF16),
            pltpu.VMEM(lead + (EDGES, rank, d), BF16),
            pltpu.VMEM(lead + (EDGES, rank, d), BF16),
            pltpu.VMEM(lead + (others, EDGES, rank, d), BF16),
            pltpu.VMEM(lead + (EDGES, rank, k), BF16),
            pltpu.VMEM(lead + (EDGES, rank, k), BF16),
            dma((count,)),
            dma(()),
            dma(()),
            dma(()),
            dma(()),
            dma((count, 2)),
            dma((others,)),
            dma(lead + (others, 2)),
            dma(()),
            dma((count,)),
        ],
        compiler_params=pltpu.CompilerParams(
            collective_id=0, has_side_effects=True, vmem_limit_bytes=40 * 2**20
        ),
    )(layers, warm_down, warm_right)


def finish_kernel(w, p, s, c, out, down, right, held, out_sem, c_sem):
    layers, d, k = w.shape
    height = piece(d, 256)
    block = piece(d, 768)
    full = p.shape[1] // ROUNDS
    last = slice((ROUNDS - 1) * full, ROUNDS * full)
    small = [
        pltpu.make_async_copy(c.at[i], dst, c_sem.at[i]) for i, dst in enumerate((down, right))
    ]
    for copy in small:
        copy.start()

    def store(l, b):
        span = pl.ds(b * block, block)
        source = w if l < EARLY else held
        return pltpu.make_async_copy(source.at[l, span], out.at[l, span], out_sem.at[l, b])

    blocks = [(l, b) for l in range(layers) for b in range(d // block)]
    for l, b in blocks:
        if l >= EARLY:
            for at in range(b * block, (b + 1) * block, height):
                cut = slice(at, at + height)
                change = lax.dot_general(
                    p[l, last, cut], s[l, last], (((0,), (0,)), ((), ())),
                    preferred_element_type=F32,
                )
                held[l, cut, :] = (w[l, cut, :].astype(F32) + change).astype(BF16)
        store(l, b).start()
    for copy in small:
        copy.wait()
    for l, b in blocks:
        store(l, b).wait()


def last_update(w0, basis, factors, combined):
    count, d, k = w0.shape
    rank = combined.shape[2]
    vmem = pl.BlockSpec(memory_space=pltpu.VMEM)
    hbm = pl.BlockSpec(memory_space=pltpu.HBM)
    dma = pltpu.SemaphoreType.DMA
    return pl.pallas_call(
        finish_kernel,
        out_shape=(
            jax.ShapeDtypeStruct((count, d, k), BF16),
            jax.ShapeDtypeStruct((count, rank, k), F32),
            jax.ShapeDtypeStruct((count, rank, k), F32),
        ),
        in_specs=[vmem, vmem, vmem, vmem],
        out_specs=(hbm, hbm, hbm),
        scratch_shapes=[
            pltpu.VMEM((count, d, k), BF16),
            dma((count, d // piece(d, 768))),
            dma((2,)),
        ],
        compiler_params=pltpu.CompilerParams(vmem_limit_bytes=24 * 2**20),
    )(w0, basis, factors, combined)


def solution(mesh):
    sizes = tuple(mesh.shape[a] for a in ("row", "col", "mp"))

    def body(weights, warm_down, warm_right):
        warm = [
            pltpu.with_memory_space_constraint(x[0, 0], pltpu.HBM)
            for x in (warm_down, warm_right)
        ]
        parts = gossip(sizes, weights[0, 0], *warm)
        new, down, right = last_update(*parts)
        return new[None, None], down[None, None], right[None, None]

    spec = P("row", "col", None, None, "mp")
    return jax.shard_map(
        body, mesh=mesh, in_specs=(spec,) * 3, out_specs=(spec,) * 3, check_vma=False
    )
```

```python
import functools

import jax
import jax.numpy as jnp
from jax import lax
from jax.experimental import pallas as pl
from jax.experimental.pallas import tpu as pltpu
from jax.sharding import PartitionSpec as P

ROUNDS = 2

step_size = 0.2
epsilon = 1e-06

MESH = pl.DeviceIdType.MESH
F32 = jnp.float32
BF16 = jnp.bfloat16
EDGES = 4


def piece(total, want):
    size = min(total, want)
    while total % size:
        size -= 128
    return size


def total(values):
    return functools.reduce(lambda a, b: a + b, values)


def orthonormal_pairs(v, rank):
    row = lax.broadcasted_iota(jnp.int32, (v.shape[0], 1), 0)
    first = row < rank
    within = jnp.where(first, row, row - rank)
    turned = [v] + [pltpu.roll(v, s, 0) for s in range(1, rank)]
    inner = [jnp.sum(v * t, axis=-1, keepdims=True) for t in turned]

    def pick(k, j):
        k, j = max(k, j), min(k, j)
        dots = inner[k - j]
        return jnp.where(first, dots[k : k + 1], dots[rank + k : rank + k + 1])

    gram = [[pick(k, j) for j in range(rank)] for k in range(rank)]
    mix, inverse = [], []
    for k in range(rank):
        ahead = [
            total([mix[j][i] * gram[k][i] for i in range(j)] + [gram[k][j]])
            * (inverse[j] * inverse[j])
            for j in range(k)
        ]
        mix.append([
            -total([ahead[j] * mix[j][i] for j in range(i + 1, k)] + [ahead[i]])
            for i in range(k)
        ])
        along = [
            total([mix[k][i] * gram[i][j] for i in range(k)] + [gram[k][j]])
            for j in range(k + 1)
        ]
        norm = total([mix[k][j] * along[j] for j in range(k)] + [along[k]])
        inverse.append(lax.rsqrt(jnp.maximum(norm, 0.0) + epsilon))
    out = None
    for s in range(rank):
        weight = jnp.zeros(row.shape, F32)
        for k in range(s, rank):
            entry = inverse[k] if s == 0 else inverse[k] * mix[k][k - s]
            weight = jnp.where(within == k, entry, weight)
        out = weight * turned[s] if s == 0 else out + weight * turned[s]
    return out


COST = {
    "own": 0.85, "far": 0.5, "forward": 0.7, "mid": 0.04, "basis": 0.62, "combine": 0.14,
    "update": 0.8,
}
ROW, COL, PART, ACROSS, ALONG, SKEW = 3.4, 2.4, 2.5, 0.4, 0.4, 0.5
ENDS = {0: 2, 1: 2}
EARLY, SOON = 2, 0.3
START, WARM, REST, LATE = 1.0, 4.2, 5.4, 2.0
RANKED = ("mid", "combine", "basis", "forward", "far", "own", "update")


def groups(r):
    return ((0, 1), (2, 3)) if r == 0 else ((0, 2), (1, 3))


def plan(layers):
    def order(r, l):
        return "ends" if l >= layers - ENDS.get(r, 0) else "sum"

    wires = {}
    now, done = 0.0, []
    ready = {("own", 0, l, 0): START + 0.3 * l for l in range(layers)}
    arrived, early, turned, based = {}, {}, [], {}

    def over(wire, t, size, latency):
        wires[wire] = max(wires.get(wire, 0.0), t) + size
        return wires[wire] + latency

    def hop(e, t):
        return over(("row", e), t, ALONG, ROW) if e % 2 == 0 else t + COL

    def across(t):
        return over("mp", t, ACROSS, PART)

    def sent(r, l, which, t):
        for g in which:
            ready["mid", r, l, g] = max(
                across(t) if order(r, l) == "sum" else hop(e, t) for e in groups(r)[g]
            )
            if name == "own":
                ready["mid", r, l, g] += SKEW

    while ready:
        held_back = set()
        if any(k[0] in ("combine", "forward") and k[1] == (k[0] == "forward") for k in ready):
            held_back = {k for k in ready if k[0] == "mid" and k[1] > 0}
        if any(k[0] == "mid" and k[1] > 0 for k in ready):
            held_back |= {k for k in ready if k[0] == "basis" and k[1] > 0}
        free = {k: t for k, t in ready.items() if k not in held_back}
        soon = [k for k, t in free.items() if t <= now]
        if soon:
            key = min(soon, key=lambda k: (RANKED.index(k[0]), ready[k], k))
            close = [k for k, t in free.items() if k[0] == "mid" and t <= now + SOON]
            if key[0] == "update" and close:
                key = min(close, key=lambda k: (ready[k], k))
        else:
            key = min(free, key=lambda k: (ready[k], k))
        name, r, l, g = key
        now = max(now, ready.pop(key)) + COST[name]
        done.append(key)
        if name == "own":
            ready["far", r, l, 0] = max(now, WARM if l == 0 else REST - (0.05 if order(r, l) == "ends" else 0.0))
            if order(r, l) == "sum":
                sent(r, l, (0,), now)
            else:
                early[l] = max(hop(e, now) for e in groups(r)[0]) + LATE
        elif name == "far" and order(r, l) == "sum":
            sent(r, l, (1,), now)
        elif name == "far":
            ready["mid", r, l, 1] = max(now, early[l])
            ready["mid", r, l, 0] = max(hop(e, now) for e in groups(r)[1])
        elif name == "forward":
            sent(r, l, (0, 1), now)
            turned += [l]
            if len(turned) == layers:
                ready.update({("update", r, i, 0): now for i in turned})
        elif name == "mid":
            got = arrived.setdefault((r, l), [])
            for e in groups(r)[g]:
                got.append(hop(e, now) if order(r, l) == "sum" else across(now))
        elif name == "basis":
            based[r, l] = now + ROW + 0.2
            if len([k for k in based if k[0] == r]) == layers:
                ready.update({("combine", a, i, 0): t for (a, i), t in based.items() if a == r})
        elif name == "combine" and r + 1 < ROUNDS:
            ready["forward", r + 1, l, 0] = now
        elif name == "combine" and l < EARLY:
            ready["update", r + 1, l, 0] = now
        if len(arrived.get((r, l), ())) == EDGES and (r == 0 or ("update", r, l, 0) in done):
            if ("basis", r, l, 0) not in done:
                ready["basis", r, l, 0] = max(arrived[r, l])
    return [(name, r, l, g, order(r, l)) for name, r, l, g in done]


def gossip_kernel(
    sizes, w_hbm, down_hbm, right_hbm, w, p_out, s_out, c_out,
    warm, warm_in, turned, q, cross, kept, held, vs, vr, ms, mr, cs, cr,
    load_sem, warm_load, warm_send, warm_recv, v_send, v_recv,
    m_send, m_recv, c_send, c_recv,
):
    rows, cols, parts = sizes
    layers, d, k = w_hbm.shape
    rank = down_hbm.shape[1]
    half = 2 * rank
    full = EDGES * rank
    row, col, part = (lax.axis_index(a) for a in ("row", "col", "mp"))
    below = {"row": lax.rem(row + 1, rows)}
    above = {"row": lax.rem(row + rows - 1, rows)}
    right = {"col": lax.rem(col + 1, cols)}
    left = {"col": lax.rem(col + cols - 1, cols)}
    peers = [{"mp": lax.rem(part + i, parts)} for i in range(1, parts)]
    sides = (below, right, above, left)

    def load(l):
        return pltpu.make_async_copy(w_hbm.at[l], w.at[l], load_sem.at[l])

    def warm_loads():
        return [
            pltpu.make_async_copy(src, warm.at[i], warm_load)
            for i, src in enumerate((down_hbm, right_hbm))
        ]

    def remote(src, dst, send, recv, target):
        return pltpu.make_async_remote_copy(
            src_ref=src, dst_ref=dst, send_sem=send, recv_sem=recv,
            device_id=target, device_id_type=MESH,
        )

    def warm_copies():
        return [
            remote(warm.at[0], warm_in.at[0], warm_send, warm_recv, below),
            remote(warm.at[1], warm_in.at[1], warm_send, warm_recv, right),
        ]

    def group(r, e):
        return [e in g for g in groups(r)].index(True)

    def m_copies(r, l, e):
        return [
            remote(ms.at[r, l, e], mr.at[r, l, i, e], m_send.at[i], m_recv.at[r, l, i, group(r, e)], t)
            for i, t in enumerate(peers)
        ]

    def v_copy(r, l, e):
        o = (e + 2) % EDGES
        return remote(vs.at[r, l, e], vr.at[r, l, o], v_send, v_recv.at[l, group(r, o)], sides[e])

    def c_copy(r, l, e):
        return remote(cs.at[r, l, e], cr.at[r, l, (e + 2) % EDGES], c_send, c_recv.at[l], sides[e])

    def m_arrive(r, l, g):
        for i, t in enumerate(peers):
            remote(
                ms.at[r, l, 0:2], mr.at[r, l, i, 0:2], m_send.at[i], m_recv.at[r, l, i, g], t
            ).wait_recv()

    def v_arrive(r, l, g):
        remote(vs.at[r, l, 0:2], vr.at[r, l, 0:2], v_send, v_recv.at[l, g], below).wait_recv()

    def c_arrive(r, l):
        remote(cs.at[r, l], cr.at[r, l], c_send, c_recv.at[l], below).wait_recv()

    def each_layer(stage):
        def step(l, carry):
            stage(l)
            return carry
        lax.fori_loop(0, layers, step, 0)

    for copy in warm_loads():
        copy.start()
    each_layer(lambda l: load(l).start())
    barrier = pltpu.get_barrier_semaphore()
    partners = list(sides) + peers
    for t in partners:
        pl.semaphore_signal(barrier, inc=1, device_id=t, device_id_type=MESH)
    width = piece(d, 768)

    def at_round(r):
        return slice(r * full, (r + 1) * full)

    def rows_of(e):
        return slice(e * rank, (e + 1) * rank)

    def launch(r, l, order, edges):
        for e in edges:
            if order == "sum":
                for copy in m_copies(r, l, e):
                    copy.start()
            else:
                v_copy(r, l, e).start()

    def products(r, l, order, factors, edges, extra=None):
        out = ms if order == "sum" else vs
        cuts = [slice(at, at + width) for at in range(0, d, width)]
        parts = []
        for cut in cuts:
            if edges == (0, 1):
                turned[l, :, cut] = w[l, cut, :].T
            parts.append(jnp.dot(factors, turned[l, :, cut], preferred_element_type=F32))
        for cut, f in zip(cuts, parts):
            if extra is not None:
                f = f + jnp.dot(extra, p_out[l, at_round(r - 1), cut], preferred_element_type=F32)
            first = edges[0] * rank
            kept[l, first : first + len(edges) * rank, cut] = f
            for i, e in enumerate(edges):
                out[r, l, e, :, cut] = f[rows_of(i)].astype(BF16)

    def own(r, l, e, order):
        load(l).wait()
        products(r, l, order, jnp.concatenate([warm[0, l], warm[1, l]], axis=0), (0, 1))
        launch(r, l, order, (0, 1))

    def far(r, l, e, order):
        if waiting:
            remote(warm, warm_in, warm_send, warm_recv, below).wait_recv()
            waiting.clear()
        products(r, l, order, jnp.concatenate([warm_in[0, l], warm_in[1, l]], axis=0), (2, 3))
        launch(r, l, order, (2, 3))

    def forward(r, l, e, order):
        products(r, l, order, q[l], (0, 1, 2, 3), cross[l])
        launch(r, l, order, (0, 2, 1, 3))

    def mid(r, l, g, order):
        if order == "sum":
            m_arrive(r, l, g)
        else:
            v_arrive(r, l, g)
        for e in groups(r)[g]:
            here = rows_of(e)
            v = kept[l, here]
            if order == "sum":
                for i in range(len(peers)):
                    v = v + mr[r, l, i, e].astype(F32)
            else:
                other = vr[r, l, e].astype(F32)
                v = v - other if e < 2 else other - v
            kept[l, here] = v
            out = vs if order == "sum" else ms
            out[r, l, e] = v.astype(BF16)
        for e in groups(r)[g]:
            if order == "sum":
                v_copy(r, l, e).start()
            else:
                for copy in m_copies(r, l, e):
                    copy.start()

    def basis(r, l, e, order):
        for g in range(2):
            if order == "sum":
                v_arrive(r, l, g)
            else:
                m_arrive(r, l, g)
        for h in range(2):
            pair = (2 * h, 2 * h + 1)
            v = kept[l, half * h : half * (h + 1)]
            if order == "sum":
                other = jnp.concatenate([vr[r, l, i].astype(F32) for i in pair], axis=0)
                v = v - other if h == 0 else other - v
            else:
                for j in range(len(peers)):
                    v = v + jnp.concatenate([mr[r, l, j, i].astype(F32) for i in pair], axis=0)
            at = r * full + half * h
            p_out[l, at : at + half] = orthonormal_pairs(v, rank).astype(BF16)
        b = jnp.dot(p_out[l, at_round(r)], w[l], preferred_element_type=F32)
        held[l] = b
        for i in range(EDGES):
            cs[r, l, i] = b[rows_of(i)].astype(BF16)
        for i in (0, 2, 1, 3):
            c_copy(r, l, i).start()

    def combine(r, l, e, order):
        c_arrive(r, l)
        far_end = [
            jnp.concatenate([cr[r, l, i].astype(F32) for i in pair], axis=0)
            for pair in ((0, 1), (2, 3))
        ]
        mine = held[l, 0:half] - far_end[0]
        theirs = far_end[1] - held[l, half:full]
        signed = (step_size * jnp.concatenate([-mine, theirs], axis=0)).astype(BF16)
        s_out[l, at_round(r)] = signed
        if r == ROUNDS - 1:
            for i in range(2):
                c_out[i, l] = mine[rows_of(i)]
        else:
            factors = jnp.concatenate([mine, theirs], axis=0).astype(BF16)
            q[l] = factors
            cross[l] = lax.dot_general(
                factors, signed, (((1,), (1,)), ((), ())), preferred_element_type=F32
            ).astype(BF16)

    height = piece(d, 256)

    def update(r, l, e, order):
        before = at_round(r - 1)
        for at in range(0, d, height):
            cut = slice(at, at + height)
            change = lax.dot_general(
                p_out[l, before, cut], s_out[l, before], (((0,), (0,)), ((), ())),
                preferred_element_type=F32,
            )
            w[l, cut, :] = (w[l, cut, :].astype(F32) + change).astype(BF16)

    waiting = [True]
    pltpu.make_async_copy(warm, warm_in, warm_load).wait()
    pl.semaphore_wait(barrier, len(partners))
    for copy in warm_copies():
        copy.start()
    stages = dict(own=own, far=far, forward=forward, mid=mid, basis=basis, combine=combine, update=update)
    for name, r, l, e, order in plan(layers):
        stages[name](r, l, e, order)

    remote(warm, warm_in, warm_send, warm_recv, below).wait_send()

    for i, t in enumerate(peers):
        remote(ms, mr.at[:, :, i], m_send.at[i], m_recv.at[0, 0, i, 0], t).wait_send()
    remote(vs, vr, v_send, v_recv.at[0, 0], below).wait_send()
    remote(cs, cr, c_send, c_recv.at[0], below).wait_send()


def gossip(sizes, layers, warm_down, warm_right):
    count, d, k = layers.shape
    rank = warm_down.shape[1]
    others = sizes[2] - 1
    full = EDGES * rank
    vmem = pl.BlockSpec(memory_space=pltpu.VMEM)
    hbm = pl.BlockSpec(memory_space=pltpu.HBM)
    dma = pltpu.SemaphoreType.DMA
    lead = (ROUNDS, count)
    return pl.pallas_call(
        functools.partial(gossip_kernel, sizes),
        out_shape=(
            jax.ShapeDtypeStruct((count, d, k), BF16),
            jax.ShapeDtypeStruct((count, ROUNDS * full, d), BF16),
            jax.ShapeDtypeStruct((count, ROUNDS * full, k), BF16),
            jax.ShapeDtypeStruct((2, count, rank, k), F32),
        ),
        in_specs=[hbm, hbm, hbm],
        out_specs=(vmem, vmem, vmem, vmem),
        scratch_shapes=[
            pltpu.VMEM((2, count, rank, k), BF16),
            pltpu.VMEM((2, count, rank, k), BF16),
            pltpu.VMEM((count, k, d), BF16),
            pltpu.VMEM((count, full, k), BF16),
            pltpu.VMEM((count, full, full), BF16),
            pltpu.VMEM((count, full, d), F32),
            pltpu.VMEM((count, full, k), F32),
            pltpu.VMEM(lead + (EDGES, rank, d), BF16),
            pltpu.VMEM(lead + (EDGES, rank, d), BF16),
            pltpu.VMEM(lead + (EDGES, rank, d), BF16),
            pltpu.VMEM(lead + (others, EDGES, rank, d), BF16),
            pltpu.VMEM(lead + (EDGES, rank, k), BF16),
            pltpu.VMEM(lead + (EDGES, rank, k), BF16),
            dma((count,)),
            dma(()),
            dma(()),
            dma(()),
            dma(()),
            dma((count, 2)),
            dma((others,)),
            dma(lead + (others, 2)),
            dma(()),
            dma((count,)),
        ],
        compiler_params=pltpu.CompilerParams(
            collective_id=0, has_side_effects=True, vmem_limit_bytes=40 * 2**20
        ),
    )(layers, warm_down, warm_right)


def finish_kernel(w, p, s, c, out, down, right, held, out_sem, c_sem):
    layers, d, k = w.shape
    height = piece(d, 256)
    block = piece(d, 768)
    full = p.shape[1] // ROUNDS
    last = slice((ROUNDS - 1) * full, ROUNDS * full)
    small = [
        pltpu.make_async_copy(c.at[i], dst, c_sem.at[i]) for i, dst in enumerate((down, right))
    ]
    for copy in small:
        copy.start()

    def store(l, b):
        span = pl.ds(b * block, block)
        source = w if l < EARLY else held
        return pltpu.make_async_copy(source.at[l, span], out.at[l, span], out_sem.at[l, b])

    blocks = [(l, b) for l in range(layers) for b in range(d // block)]
    for l, b in blocks:
        if l >= EARLY:
            for at in range(b * block, (b + 1) * block, height):
                cut = slice(at, at + height)
                change = lax.dot_general(
                    p[l, last, cut], s[l, last], (((0,), (0,)), ((), ())),
                    preferred_element_type=F32,
                )
                held[l, cut, :] = (w[l, cut, :].astype(F32) + change).astype(BF16)
        store(l, b).start()
    for copy in small:
        copy.wait()
    for l, b in blocks:
        store(l, b).wait()


def last_update(w0, basis, factors, combined):
    count, d, k = w0.shape
    rank = combined.shape[2]
    vmem = pl.BlockSpec(memory_space=pltpu.VMEM)
    hbm = pl.BlockSpec(memory_space=pltpu.HBM)
    dma = pltpu.SemaphoreType.DMA
    return pl.pallas_call(
        finish_kernel,
        out_shape=(
            jax.ShapeDtypeStruct((count, d, k), BF16),
            jax.ShapeDtypeStruct((count, rank, k), F32),
            jax.ShapeDtypeStruct((count, rank, k), F32),
        ),
        in_specs=[vmem, vmem, vmem, vmem],
        out_specs=(hbm, hbm, hbm),
        scratch_shapes=[
            pltpu.VMEM((count, d, k), BF16),
            dma((count, d // piece(d, 768))),
            dma((2,)),
        ],
        compiler_params=pltpu.CompilerParams(vmem_limit_bytes=24 * 2**20),
    )(w0, basis, factors, combined)


def solution(mesh):
    sizes = tuple(mesh.shape[a] for a in ("row", "col", "mp"))

    def body(weights, warm_down, warm_right):
        warm = [
            pltpu.with_memory_space_constraint(x[0, 0], pltpu.HBM)
            for x in (warm_down, warm_right)
        ]
        parts = gossip(sizes, weights[0, 0], *warm)
        new, down, right = last_update(*parts)
        return new[None, None], down[None, None], right[None, None]

    spec = P("row", "col", None, None, "mp")
    return jax.shard_map(
        body, mesh=mesh, in_specs=(spec,) * 3, out_specs=(spec,) * 3, check_vma=False
    )
```
